512 devices in a mesh: obs: 16 (over x, y), patch: 32 (over z, core).
Axes of the slice: x: 4, y: 4, z: 16, core: 2. Of those that a mesh axis runs over, the one named last changes fastest.
Arguments:
- green: float32 [20480, 20480], P('obs', 'patch'), may hold values from -0.0390625 to 0.0390625
- data: float32 [20480, 128], P('obs'), may hold values from -6 to 6
- neighbours: int32 [3, 20480], P(None, 'patch'), may hold values from 0 to 20479, as said below
- reg_weight: float32 [128], replicated, may hold values from 0.5 to 2
Outputs:
- slip: float32 [20480, 128], P('patch')
The draws below stay inside these ranges and needn't reach their ends.
Inputs may be any that keep to these rules, and one draw needn't show every extreme that they name: `neighbours`: entry (k, i) is a patch within 128 of i; an entry equal to i is padding. Distance 128 is reached in every draw.
All inputs are finite; a program needn't handle non-finite values.
Results may differ from the reference program's by a relative error of at most 0.0001.
Values sent between devices are 32-bit elements; how exact they have to be, the bound alone decides.
A program may use at most 64 MiB of HBM per device.

```python
import math
import jax
import jax.numpy as jnp
from jax import lax

EPOCHS = 128
BAND = 128
ITERS = 3
OBS = 20480
NPATCH = 20480


def draw_neighbours(key, part):
    key_offsets = jax.random.fold_in(key, 11)
    key_padding = jax.random.fold_in(key, 12)
    offsets = jax.random.randint(key_offsets, (3, NPATCH), -BAND, BAND + 1)
    padding = jax.random.randint(key_padding, (3, NPATCH), 0, 4) == 0
    offsets = jnp.where(padding, 0, offsets)
    indices = jnp.arange(NPATCH, dtype=jnp.int32)
    marked = indices % 37 == 5
    offsets = offsets.at[0].set(jnp.where(marked, -BAND, offsets[0]))
    offsets = offsets.at[1].set(jnp.where(marked, BAND, offsets[1]))
    return jnp.clip(indices[None, :] + offsets, 0, NPATCH - 1).astype(jnp.int32)


def level_of(key, extent, split, least, largest):
    level = 1.0
    for position, parts in split:
        draws = jax.random.uniform(jax.random.fold_in(jax.random.fold_in(key, 6), position), (parts,), jnp.float32, least / len(split), largest / len(split))
        level = level * jnp.repeat(jnp.exp(draws), extent[position] // parts).reshape((-1,) + (1,) * (len(extent) - 1 - position))
    return level


def gaussian(stream_key, dims, spread, most, shards=(), kind=jnp.bfloat16):
    loudness = level_of(stream_key, dims, shards, -0.22, 0.18) if shards else 1.0
    array = jax.random.normal(stream_key, dims, jnp.float32) * spread * loudness
    return jnp.minimum(jnp.maximum(array, -most), most).astype(kind)


def setup_inputs(seed: int = 0) -> dict:
    seeds = jax.random.split(jax.random.key(seed), 5)
    green = gaussian(seeds[0], (OBS, NPATCH), NPATCH ** -0.5, 0.0390625, ((0, 16), (1, 32)), jnp.float32)
    data = gaussian(seeds[1], (OBS, EPOCHS), 1.0, 6.0, ((0, 16),), jnp.float32)
    neighbours = draw_neighbours(jax.random.fold_in(seeds[4], 71), 0)
    reg_weight = jnp.clip(jnp.exp(jax.random.uniform(seeds[3], (EPOCHS,), jnp.float32, math.log(0.5), math.log(2.0))), 0.5, 2.0)
    return {"green": green, "data": data, "neighbours": neighbours, "reg_weight": reg_weight}


def laplace(field, neighbours):
    return 4.0 * field - field[neighbours[0]] - field[neighbours[1]] - field[neighbours[2]]


def laplace_t(values, neighbours):
    result = 4.0 * values
    for slot in range(3):
        result = result.at[neighbours[slot]].add(-values)
    return result


def transposed(green, residual):
    return lax.dot_general(green, residual, (((0,), (0,)), ((), ())), precision=lax.Precision.HIGHEST, preferred_element_type=jnp.float32)


def reference(green, data, neighbours, reg_weight):
    slip = jnp.zeros((NPATCH, EPOCHS), jnp.float32)
    residual = data
    reg_resid = jnp.zeros((NPATCH, EPOCHS), jnp.float32)
    gradient = transposed(green, data)
    grad_norm = jnp.sum(gradient * gradient, axis=0)
    direction = gradient
    for iteration in range(ITERS):
        image = jnp.dot(green, direction, precision=lax.Precision.HIGHEST, preferred_element_type=jnp.float32)
        reg_image = reg_weight * laplace(direction, neighbours)
        curvature = jnp.sum(image * image, axis=0) + jnp.sum(reg_image * reg_image, axis=0)
        step_size = grad_norm / curvature
        slip = slip + step_size * direction
        if iteration + 1 < ITERS:
            residual = residual - step_size * image
            reg_resid = reg_resid - step_size * reg_image
            gradient = transposed(green, residual) + reg_weight * laplace_t(reg_resid, neighbours)
            next_norm = jnp.sum(gradient * gradient, axis=0)
            direction = gradient + (next_norm / grad_norm) * direction
            grad_norm = next_norm
    return slip
```

```python
import jax
import jax.numpy as jnp
from jax import lax
from jax.experimental import pallas as pl
from jax.experimental.pallas import tpu as pltpu
from jax.sharding import Mesh
from jax.sharding import PartitionSpec as P

ITERS = 3
NX, NY, NZ = 4, 4, 16
XY = NX * NY
OBS = ("x", "y")
PATCH = ("z", "c")
F32, BF16 = jnp.float32, jnp.bfloat16
MESH = pl.DeviceIdType.MESH

R = 40
HALO = 7
KWIN = 384
JWIN = 640
OFFH = 256

SEMS = (
    ["g0", "g1", "g2", "g3", "g4", "data", "s_off", "r_offl", "r_offr", "s_xy", "r_xy", "s_xs", "r_xs", "s_xg", "r_xg"]
    + ["s_pa", "r_pa", "s_pair", "r_pair", "s_rs", "r_relp", "r_relm", "r_dir", "r_fin", "s_sa", "r_sa"]
    + ["s_hl", "s_hr", "r_hl", "r_hr", "s_ag", "r_aga", "r_agb", "r_ag6", "r_ag7", "s_pb", "r_pb", "s_sb", "r_sb"]
    + ["s_pag", "r_pag"]
)
SEM = {name: place for place, name in enumerate(SEMS)}


def split(value):
    high = value.astype(BF16)
    low = (value - high.astype(F32)).astype(BF16)
    return high, low


def halves(value):
    return jnp.concatenate(split(value), axis=-1)


def folded(value):
    return value[:, :128] + value[:, 128:]


def dot(a, b):
    return jnp.dot(a, b, preferred_element_type=F32)


def kernel(
    green, data, neighbours, weight, out,
    gf, ghi, glo, thi, tlo, g2, im2, part, pairb, relp, relm, dirb, fin, img, q, xyr, gext, d,
    imgown, ldown, rown, offl, lx, lxt, sca, scb, xs, pab, snd, vals, sems,
):
    x, y, z, c = (lax.axis_index(a) for a in ("x", "y", "z", "c"))
    j = x * NY + y
    sign = 1 - 2 * c
    partner = (x, y, z, 1 - c)

    def ring(step):
        return lax.rem(z + sign * step + 2 * NZ, NZ)

    def along(step):
        return (x, y, ring(step), c)

    def wrapped(place):
        return lax.rem(place + NZ, NZ)

    before = (x, y, wrapped(z - 1 + c), 1 - c)
    after = (x, y, wrapped(z + c), 1 - c)

    def plane():
        for dx in range(NX):
            for dy in range(NY):
                if dx or dy:
                    px, py = lax.rem(x + dx, NX), lax.rem(y + dy, NY)
                    yield px * NY + py, (px, py, z, c)

    def copy(src, dst, s, r, to):
        return pltpu.make_async_remote_copy(
            src_ref=src, dst_ref=dst, send_sem=sems.at[SEM[s]], recv_sem=sems.at[SEM[r]],
            device_id=to, device_id_type=MESH,
        )

    def put(src, dst, s, r, to):
        copy(src, dst, s, r, to).start()

    def got(ref, r):
        copy(ref, ref, "s_xy", r, partner).wait_recv()

    def sent(ref, s):
        copy(ref, ref, s, "r_xy", partner).wait_send()

    loads = [
        pltpu.make_async_copy(green.at[pl.ds(256 * i, 256)], gf.at[pl.ds(256 * i, 256)], sems.at[SEM["g0"] + i])
        for i in range(5)
    ]
    load_data = pltpu.make_async_copy(data, img, sems.at[SEM["data"]])
    for load in loads:
        load.start()
    load_data.start()

    cols = neighbours.shape[1]
    base = (2 * z + c) * cols
    ids = base + lax.broadcasted_iota(jnp.int32, neighbours.shape, 1)
    offl[...] = jnp.zeros_like(offl)
    offl[0:3, OFFH : OFFH + cols] = (neighbours[...] - ids).astype(F32)
    for ref in (gext, d, imgown, ldown, rown, sca, scb, xs, vals):
        ref[...] = jnp.zeros_like(ref)
    out[...] = jnp.zeros_like(out)
    vals[1:2] = jnp.ones((1, 1, 128), F32)

    barrier = pltpu.get_barrier_semaphore()
    greeted = [along(k) for k in range(1, NZ)] + [to for _, to in plane()]
    greeted += [partner, (x, y, wrapped(z - 1 + 2 * c), 1 - c)]
    for to in greeted:
        pl.semaphore_signal(barrier, inc=1, device_id=to, device_id_type=MESH)

    for i in range(5):
        loads[i].wait()
        for k in range(2):
            rows = pl.ds(256 * i + 128 * k, 128)
            block = gf[rows, :]
            ghi[rows, :], glo[rows, :] = split(block)
            thi[:, rows], tlo[:, rows] = split(block.T)
    load_data.wait()

    pl.semaphore_wait(barrier, len(greeted))
    put(offl.at[:, pl.ds(cols, OFFH)], offl.at[:, pl.ds(0, OFFH)], "s_off", "r_offl", after)
    put(offl.at[:, pl.ds(OFFH, OFFH)], offl.at[:, pl.ds(OFFH + cols, OFFH)], "s_off", "r_offr", before)

    def forward(half):
        def tile(i, _):
            rows = pl.ds(pl.multiple_of(half * 640 + i * 160, 160), 160)
            both = dot(ghi[rows, :], g2[...]) + dot(glo[rows, :], g2[...])
            part[half, pl.ds(4 * i, 4)] = folded(both).reshape(4, R, 128)
            return 0

        lax.fori_loop(0, 4, tile, 0)

    def back(half, add):
        def convert(i, _):
            rows = pl.ds(pl.multiple_of(i * 160, 160), 160)
            im2[rows, :] = halves(img[half, pl.ds(4 * i, 4)].reshape(160, 128))
            return 0

        lax.fori_loop(0, 4, convert, 0)
        depth = pl.ds(pl.multiple_of(half * 640, 128), 640)

        def tile(i, _):
            rows = pl.ds(pl.multiple_of(i * 160, 160), 160)
            both = dot(thi[rows, depth], im2[...]) + dot(tlo[rows, depth], im2[...])
            value = folded(both).reshape(4, R, 128)
            place = pl.ds(4 * i, 4)
            q[place] = q[place] + value if add else value
            return 0

        lax.fori_loop(0, 4, tile, 0)

    def exchange_curvature():
        xs[pl.ds(j, 1)] = jnp.sum(scb[...], axis=0, keepdims=True)
        for _, to in plane():
            put(xs.at[j], xs.at[j], "s_xs", "r_xs", to)

    def curvature():
        got(xs.at[pl.ds(0, XY - 1)], "r_xs")
        return jnp.sum(xs[...], axis=0)

    def step_on(scale):
        def add(i, _):
            out[i] = out[i] + scale * d[i]
            return 0

        lax.fori_loop(0, XY, add, 0)

    def build_l():
        got(offl.at[:, pl.ds(0, OFFH)], "r_offl")
        got(offl.at[:, pl.ds(0, OFFH)], "r_offr")
        pick = (
            lax.broadcasted_iota(jnp.int32, (8, 128), 0) == lax.broadcasted_iota(jnp.int32, (8, 128), 1)
        ).astype(F32)
        turned = lax.dot_general(
            offl[...].astype(BF16), pick.astype(BF16), (((0,), (0,)), ((), ())), preferred_element_type=F32
        )
        gf[0:1152, 0:128] = turned
        first = base + R * j - 160
        column = lax.broadcasted_iota(jnp.int32, (16, JWIN), 1).astype(F32)

        def rows16(i, _):
            shift = gf[pl.ds(pl.multiple_of(96 + R * j + 16 * i, 8), 16), 0:128]
            row = 16 * i + lax.broadcasted_iota(jnp.int32, (16, 1), 0)
            place = (row + 120).astype(F32)
            value = jnp.where(column == place, 4.0, 0.0)
            for slot in range(3):
                value = value - jnp.where(column == place + shift[:, slot : slot + 1], 1.0, 0.0)
            known = jnp.logical_and(first + row >= 0, first + row < cols * 2 * NZ)
            value = value * known.astype(F32)
            lx[pl.ds(pl.multiple_of(16 * i, 16), 16), :] = value.astype(BF16)
            return 0

        lax.fori_loop(0, KWIN // 16, rows16, 0)
        lxt[...] = lx[:, 256:384].astype(F32).T.astype(BF16)

    def body(it, _):
        back(c, False)

        @pl.when(it > 0)
        def _():
            got(img.at[0], "r_pag")

        back(1 - c, True)

        @pl.when(it > 0)
        def _():
            sent(img.at[0], "s_pag")
            got(scb.at[pl.ds(0, NZ - 1)], "r_sb")

        exchange_curvature()
        for other, to in plane():
            put(q.at[other], xyr.at[j], "s_xy", "r_xy", to)
        xyr[j] = q[j]
        alpha = jnp.where(it == 0, -1.0, vals[0] / curvature())
        got(xyr.at[pl.ds(0, XY - 1)], "r_xy")
        total = jnp.sum(xyr[...], axis=0) + weight[...] * weight[...] * rown[...]
        gext[HALO + j] = gext[HALO + j] - alpha * total
        for _, to in plane():
            put(gext.at[HALO + j], gext.at[HALO + j], "s_xg", "r_xg", to)
        step_on(alpha)
        got(gext.at[pl.ds(0, XY - 1)], "r_xg")

        def convert(i, square):
            value = gext[pl.ds(HALO + 4 * i, 4)].reshape(160, 128)
            g2[pl.ds(pl.multiple_of(160 * i, 160), 160), :] = halves(value)
            return square + jnp.sum(value * value, axis=0, keepdims=True)

        square = lax.fori_loop(0, 4, convert, jnp.zeros((1, 128), F32))
        snd[0] = square
        put(snd.at[0], pab.at[0], "s_pa", "r_pa", partner)
        forward(1 - c)
        put(part.at[1 - c], pairb, "s_pair", "r_pair", partner)
        forward(c)
        got(pab.at[0], "r_pa")
        sca[z] = square + pab[0]
        got(pairb, "r_pair")

        def add_pair(i, _):
            part[c, i] = part[c, i] + pairb[i]
            return 0

        lax.fori_loop(0, NZ, add_pair, 0)

        mine = part.at[c]
        for e in (8, 7, 6, 5):
            put(mine.at[ring(e)], relp.at[e - 5], "s_rs", "r_relp", along(e - 4))
            if e < 8:
                put(mine.at[ring(-e)], relm.at[e - 5], "s_rs", "r_relm", along(4 - e))
        for e in (3, 2, 1):
            put(mine.at[ring(e)], dirb.at[e - 1], "s_rs", "r_dir", along(e))
            put(mine.at[ring(-e)], dirb.at[e + 2], "s_rs", "r_dir", along(-e))
        for k in range(1, NZ):
            put(sca.at[z], sca.at[z], "s_sa", "r_sa", along(k))

        @pl.when(j < HALO)
        def _():
            put(gext.at[pl.ds(XY, HALO)], gext.at[pl.ds(0, HALO)], "s_hl", "r_hl", after)

        @pl.when(j >= XY - HALO)
        def _():
            put(gext.at[pl.ds(HALO, HALO)], gext.at[pl.ds(HALO + XY, HALO)], "s_hr", "r_hr", before)

        got(relp, "r_relp")
        part[c, ring(4)] = part[c, ring(4)] + jnp.sum(relp[...], axis=0)
        put(mine.at[ring(4)], fin.at[0], "s_rs", "r_fin", along(4))
        got(relm, "r_relm")
        part[c, ring(-4)] = part[c, ring(-4)] + jnp.sum(relm[...], axis=0)
        put(mine.at[ring(-4)], fin.at[1], "s_rs", "r_fin", along(-4))

        got(sca.at[pl.ds(0, NZ - 1)], "r_sa")
        norm = jnp.sum(sca[...], axis=0)
        beta = norm / vals[1]
        vals[0] = norm
        vals[1] = norm
        got(dirb, "r_dir")
        got(fin, "r_fin")
        image = part[c, z] + jnp.sum(dirb[...], axis=0) + jnp.sum(fin[...], axis=0) + beta * imgown[...]
        imgown[...] = image

        @pl.when(it < ITERS - 1)
        def _():
            img[c, z] = image
            for e in (4, 3, 2, 1):
                for way in (e, -e):
                    r = {4: "r_aga", -4: "r_agb"}.get(way, "r_ag6")
                    put(img.at[c, z], img.at[c, z], "s_ag", r, along(way))

        @pl.when(it == 0)
        def _():
            build_l()

        @pl.when(j < HALO)
        def _():
            got(gext.at[pl.ds(0, HALO)], "r_hl")
            sent(gext.at[pl.ds(0, HALO)], "s_hl")

        @pl.when(j >= XY - HALO)
        def _():
            got(gext.at[pl.ds(0, HALO)], "r_hr")
            sent(gext.at[pl.ds(0, HALO)], "s_hr")

        window = gext[pl.ds(j, XY)].reshape(JWIN, 128)
        lg = folded(dot(lx[...], halves(window)))
        rg = folded(dot(lxt[...], halves(lg)))[24 : 24 + R]
        ld = lg[160 : 160 + R] + beta * ldown[...]
        ldown[...] = ld
        rown[...] = rg + beta * rown[...]
        share = jnp.sum(image * image, axis=0, keepdims=True)
        share = share + weight[...] * weight[...] * jnp.sum(ld * ld, axis=0, keepdims=True)
        snd[1] = share
        put(snd.at[1], pab.at[1], "s_pb", "r_pb", partner)

        def turn(i, _):
            d[i] = gext[HALO + i] + beta * d[i]
            return 0

        lax.fori_loop(0, XY, turn, 0)
        got(pab.at[1], "r_pb")
        scb[z] = share + pab[1]
        for k in range(1, NZ):
            put(scb.at[z], scb.at[z], "s_sb", "r_sb", along(k))

        @pl.when(it < ITERS - 1)
        def _():
            got(img.at[c, 0], "r_aga")
            for e in (4, 3, 2, 1):
                put(img.at[c, ring(-4)], img.at[c, ring(-4)], "s_ag", "r_ag7", along(e))
            got(img.at[c, 0], "r_agb")
            for e in (3, 2, 1):
                put(img.at[c, ring(4)], img.at[c, ring(4)], "s_ag", "r_ag7", along(-e))
            got(img.at[c, pl.ds(0, 6)], "r_ag6")
            got(img.at[c, pl.ds(0, 7)], "r_ag7")
            put(img.at[c], img.at[c], "s_pag", "r_pag", partner)
            sent(img.at[c, pl.ds(0, 15)], "s_ag")

        sent(xyr.at[pl.ds(0, XY - 1)], "s_xy")
        sent(xs.at[pl.ds(0, XY - 1)], "s_xs")
        sent(gext.at[pl.ds(0, XY - 1)], "s_xg")
        sent(snd.at[0], "s_pa")
        sent(snd.at[1], "s_pb")
        sent(pairb, "s_pair")
        sent(pairb.at[pl.ds(0, NZ - 1)], "s_rs")
        sent(sca.at[pl.ds(0, NZ - 1)], "s_sa")
        sent(scb.at[pl.ds(0, NZ - 1)], "s_sb")
        return 0

    lax.fori_loop(0, ITERS, body, 0)

    got(scb.at[pl.ds(0, NZ - 1)], "r_sb")
    exchange_curvature()
    step_on(vals[0] / curvature())
    sent(xs.at[pl.ds(0, XY - 1)], "s_xs")
    sent(offl.at[:, pl.ds(0, 2 * OFFH)], "s_off")


def shards(green, data, neighbours, reg_weight):
    rows, cols = green.shape
    chunks = (XY, R, 128)
    vmem = pl.BlockSpec(memory_space=pltpu.VMEM)
    hbm = pl.BlockSpec(memory_space=pl.ANY)
    scratch = [
        ((rows, cols), F32),
        ((rows, cols), BF16), ((rows, cols), BF16), ((cols, rows), BF16), ((cols, rows), BF16),
        ((640, 256), BF16), ((640, 256), BF16),
        ((2, *chunks), F32), (chunks, F32),
        ((4, R, 128), F32), ((3, R, 128), F32), ((6, R, 128), F32), ((2, R, 128), F32),
        ((2, *chunks), F32), (chunks, F32), (chunks, F32),
        ((2 * HALO + XY + 1, R, 128), F32), (chunks, F32),
        ((R, 128), F32), ((R, 128), F32), ((R, 128), F32),
        ((8, 2 * OFFH + cols), F32), ((KWIN, JWIN), BF16), ((128, KWIN), BF16),
        ((NZ, 1, 128), F32), ((NZ, 1, 128), F32), ((XY, 1, 128), F32),
        ((2, 1, 128), F32), ((2, 1, 128), F32), ((2, 1, 128), F32),
    ]
    result = pl.pallas_call(
        kernel,
        out_shape=jax.ShapeDtypeStruct(chunks, F32),
        in_specs=[hbm, hbm, vmem, vmem],
        out_specs=vmem,
        scratch_shapes=[pltpu.VMEM(shape, kind) for shape, kind in scratch]
        + [pltpu.SemaphoreType.DMA((len(SEMS),))],
        compiler_params=pltpu.CompilerParams(
            collective_id=0, has_side_effects=True, vmem_limit_bytes=48 * 1024 * 1024
        ),
    )(green, data.reshape(2, *chunks), neighbours, reg_weight.reshape(1, 128))
    return result.reshape(cols, 128)


def solution(mesh):
    whole = Mesh(mesh.devices.reshape(NX, NY, NZ, 2), ("x", "y", "z", "c"))
    in_specs = (P(OBS, PATCH), P(OBS, None), P(None, PATCH), P())
    return jax.shard_map(
        shards, mesh=whole, in_specs=in_specs, out_specs=P(PATCH, None), check_vma=False
    )
```

```python
import jax
import jax.numpy as jnp
from jax import lax
from jax.experimental import pallas as pl
from jax.experimental.pallas import tpu as pltpu
from jax.sharding import Mesh
from jax.sharding import PartitionSpec as P

ITERS = 3
NX, NY, NZ = 4, 4, 16
XY = NX * NY
OBS = ("x", "y")
PATCH = ("z", "c")
F32, BF16 = jnp.float32, jnp.bfloat16
MESH = pl.DeviceIdType.MESH

R = 40
HALO = 7
KWIN = 384
JWIN = 640
OFFH = 256

SEMS = (
    ["g0", "g1", "g2", "g3", "g4", "data", "nb", "w", "s_off", "r_offl", "r_offr", "s_xy", "r_xy", "s_xs", "r_xs", "s_xg", "r_xg"]
    + ["s_pa", "r_pa", "s_pair", "r_pair", "s_rs", "r_relp", "r_relm", "r_dir", "r_fin", "s_sa", "r_sa"]
    + ["s_hl", "s_hr", "r_hl", "r_hr", "s_ag", "r_aga", "r_agb", "r_ag6", "r_ag7", "s_sb", "r_sb"]
    + ["s_pag", "r_pag"]
)
SEM = {name: place for place, name in enumerate(SEMS)}


def hops(offset):
    return sum(min(step, size - step) for step, size in zip(offset, (NX, NY)))


FAR_RING = sorted(range(1, NZ), key=lambda k: min(k, NZ - k), reverse=True)
FARTHEST_FIRST = sorted(
    ((dx, dy) for dx in range(NX) for dy in range(NY) if dx or dy), key=hops, reverse=True
)


def split(value):
    high = value.astype(BF16)
    low = (value - high.astype(F32)).astype(BF16)
    return high, low


def halves(value):
    return jnp.concatenate(split(value), axis=-1)


def folded(value):
    return value[:, :128] + value[:, 128:]


def dot(a, b):
    return jnp.dot(a, b, preferred_element_type=F32)


def kernel(
    green, data, neighbours, reg_weight, out,
    gf, ghi, glo, thi, tlo, g2, im2, part, pairb, relp, relm, dirb, fin, img, q, xyr, gext, d,
    imgown, ldown, rown, offl, lx, lxt, sca, scb, xs, pab, snd, vals, table, weight, sems,
):
    x, y, z, c = (lax.axis_index(a) for a in ("x", "y", "z", "c"))
    j = x * NY + y
    sign = 1 - 2 * c
    partner = (x, y, z, 1 - c)

    def ring(step):
        return lax.rem(z + sign * step + 2 * NZ, NZ)

    def along(step):
        return (x, y, ring(step), c)

    def wrapped(place):
        return lax.rem(place + NZ, NZ)

    before = (x, y, wrapped(z - 1 + c), 1 - c)
    after = (x, y, wrapped(z + c), 1 - c)

    def plane():
        for dx, dy in FARTHEST_FIRST:
            px, py = lax.rem(x + dx, NX), lax.rem(y + dy, NY)
            yield px * NY + py, (px, py, z, c)

    def copy(src, dst, s, r, to):
        return pltpu.make_async_remote_copy(
            src_ref=src, dst_ref=dst, send_sem=sems.at[SEM[s]], recv_sem=sems.at[SEM[r]],
            device_id=to, device_id_type=MESH,
        )

    def put(src, dst, s, r, to):
        copy(src, dst, s, r, to).start()

    def got(ref, r):
        copy(ref, ref, "s_xy", r, partner).wait_recv()

    def sent(ref, s):
        copy(ref, ref, s, "r_xy", partner).wait_send()

    loads = [
        pltpu.make_async_copy(green.at[pl.ds(256 * i, 256)], gf.at[pl.ds(256 * i, 256)], sems.at[SEM["g0"] + i])
        for i in range(5)
    ]
    load_data = pltpu.make_async_copy(data, img, sems.at[SEM["data"]])
    load_table = pltpu.make_async_copy(neighbours, table, sems.at[SEM["nb"]])
    load_weight = pltpu.make_async_copy(reg_weight, weight, sems.at[SEM["w"]])
    load_table.start()
    for load in loads:
        load.start()
    load_data.start()
    load_weight.start()

    cols = neighbours.shape[1]
    base = (2 * z + c) * cols
    for ref in (gext, d, imgown, ldown, rown, sca, scb, xs, offl):
        ref[...] = jnp.zeros_like(ref)
    vals[0:1] = jnp.full((1, 1, 128), -1.0, F32)
    vals[1:2] = jnp.ones((1, 1, 128), F32)
    load_table.wait()
    ids = base + lax.broadcasted_iota(jnp.int32, table.shape, 1)
    offl[0:3, OFFH : OFFH + cols] = (table[...] - ids).astype(F32)

    barrier = pltpu.get_barrier_semaphore()
    greeted = [along(k) for k in range(1, NZ)] + [to for _, to in plane()]
    greeted += [partner] + [(x, y, ring(k), 1 - c) for k in range(1, NZ)]
    for to in greeted:
        pl.semaphore_signal(barrier, inc=1, device_id=to, device_id_type=MESH)

    out[...] = jnp.zeros_like(out)
    for i in range(5):
        loads[i].wait()
        for k in range(2):
            place = 2 * i + k
            high, low = split(gf[pl.ds(128 * place, 128), :].T)
            half, columns = place // 5, pl.ds(128 * (place % 5), 128)
            thi[half, :, columns], tlo[half, :, columns] = high, low
    load_weight.wait()
    load_data.wait()

    def forward(half):
        def tile(i, _):
            rows = pl.ds(pl.multiple_of(half * 640 + i * 160, 160), 160)
            both = dot(ghi[rows, :], g2[...]) + dot(glo[rows, :], g2[...])
            part[half, pl.ds(4 * i, 4)] = folded(both).reshape(4, R, 128)
            return 0

        lax.fori_loop(0, 4, tile, 0)

    def back(half, add):
        def convert(i, _):
            rows = pl.ds(pl.multiple_of(i * 160, 160), 160)
            im2[rows, :] = halves(img[half, pl.ds(4 * i, 4)].reshape(160, 128))
            return 0

        lax.fori_loop(0, 4, convert, 0)
        def tile(i, _):
            rows = pl.ds(pl.multiple_of(i * 160, 160), 160)
            both = dot(thi[half, rows, :], im2[...]) + dot(tlo[half, rows, :], im2[...])
            value = folded(both).reshape(4, R, 128)
            place = pl.ds(4 * i, 4)
            q[place] = q[place] + value if add else value
            return 0

        lax.fori_loop(0, 4, tile, 0)

    def split_rows():
        def tile(i, _):
            rows = pl.ds(pl.multiple_of(i * 128, 128), 128)
            ghi[rows, :], glo[rows, :] = split(gf[rows, :])
            return 0

        lax.fori_loop(0, 10, tile, 0)

    def exchange_curvature():
        got(scb.at[pl.ds(0, 2 * NZ - 1)], "r_sb")
        xs[pl.ds(j, 1)] = jnp.sum(scb[...], axis=0, keepdims=True)
        for _, to in plane():
            put(xs.at[j], xs.at[j], "s_xs", "r_xs", to)

    def curvature():
        got(xs.at[pl.ds(0, XY - 1)], "r_xs")
        return jnp.sum(xs[...], axis=0)

    def step_on(scale):
        def add(i, _):
            out[i] = out[i] + scale * d[i]
            return 0

        lax.fori_loop(0, XY, add, 0)

    def build_l():
        got(offl.at[:, pl.ds(0, OFFH)], "r_offl")
        got(offl.at[:, pl.ds(0, OFFH)], "r_offr")
        pick = (
            lax.broadcasted_iota(jnp.int32, (8, 128), 0) == lax.broadcasted_iota(jnp.int32, (8, 128), 1)
        ).astype(F32)
        turned = lax.dot_general(
            offl[...].astype(BF16), pick.astype(BF16), (((0,), (0,)), ((), ())), preferred_element_type=F32
        )
        gf[0:1152, 0:128] = turned
        first = base + R * j - 160
        column = lax.broadcasted_iota(jnp.int32, (16, JWIN), 1).astype(F32)

        def rows16(i, _):
            shift = gf[pl.ds(pl.multiple_of(96 + R * j + 16 * i, 8), 16), 0:128]
            row = 16 * i + lax.broadcasted_iota(jnp.int32, (16, 1), 0)
            place = (row + 120).astype(F32)
            value = jnp.where(column == place, 4.0, 0.0)
            for slot in range(3):
                value = value - jnp.where(column == place + shift[:, slot : slot + 1], 1.0, 0.0)
            known = jnp.logical_and(first + row >= 0, first + row < cols * 2 * NZ)
            value = value * known.astype(F32)
            lx[pl.ds(pl.multiple_of(16 * i, 16), 16), :] = value.astype(BF16)
            return 0

        lax.fori_loop(0, KWIN // 16, rows16, 0)
        lxt[...] = lx[:, 256:384].astype(F32).T.astype(BF16)

    def body(it, _):
        back(c, False)

        @pl.when(it > 0)
        def _():
            got(img.at[0], "r_pag")

        back(1 - c, True)

        @pl.when(it > 0)
        def _():
            sent(img.at[0], "s_pag")

        @pl.when(it == 0)
        def _():
            pl.semaphore_wait(barrier, len(greeted))
            put(offl.at[:, pl.ds(cols, OFFH)], offl.at[:, pl.ds(0, OFFH)], "s_off", "r_offl", after)
            put(offl.at[:, pl.ds(OFFH, OFFH)], offl.at[:, pl.ds(OFFH + cols, OFFH)], "s_off", "r_offr", before)

        for other, to in plane():
            put(q.at[other], xyr.at[j], "s_xy", "r_xy", to)
        xyr[j] = q[j]

        @pl.when(it > 0)
        def _():
            exchange_curvature()
            vals[0] = vals[1] / curvature()

        @pl.when(it == 0)
        def _():
            split_rows()

        alpha = vals[0]
        got(xyr.at[pl.ds(0, XY - 1)], "r_xy")
        total = jnp.sum(xyr[...], axis=0) + weight[...] * weight[...] * rown[...]
        gext[HALO + j] = gext[HALO + j] - alpha * total
        for _, to in plane():
            put(gext.at[HALO + j], gext.at[HALO + j], "s_xg", "r_xg", to)
        step_on(alpha)
        got(gext.at[pl.ds(0, XY - 1)], "r_xg")

        @pl.when(j < HALO)
        def _():
            put(gext.at[pl.ds(XY, HALO)], gext.at[pl.ds(0, HALO)], "s_hl", "r_hl", after)

        @pl.when(j >= XY - HALO)
        def _():
            put(gext.at[pl.ds(HALO, HALO)], gext.at[pl.ds(HALO + XY, HALO)], "s_hr", "r_hr", before)

        def convert(i, square):
            value = gext[pl.ds(HALO + 4 * i, 4)].reshape(160, 128)
            g2[pl.ds(pl.multiple_of(160 * i, 160), 160), :] = halves(value)
            return square + jnp.sum(value * value, axis=0, keepdims=True)

        square = lax.fori_loop(0, 4, convert, jnp.zeros((1, 128), F32))
        snd[0] = square
        put(snd.at[0], pab.at[0], "s_pa", "r_pa", partner)
        forward(1 - c)
        put(part.at[1 - c], pairb, "s_pair", "r_pair", partner)
        forward(c)
        got(pab.at[0], "r_pa")
        sca[z] = square + pab[0]
        got(pairb, "r_pair")

        def add_pair(i, _):
            part[c, i] = part[c, i] + pairb[i]
            return 0

        lax.fori_loop(0, NZ, add_pair, 0)

        mine = part.at[c]
        for e in (8, 7, 6, 5):
            put(mine.at[ring(e)], relp.at[e - 5], "s_rs", "r_relp", along(e - 4))
            if e < 8:
                put(mine.at[ring(-e)], relm.at[e - 5], "s_rs", "r_relm", along(4 - e))
        for e in (3, 2, 1):
            put(mine.at[ring(e)], dirb.at[e - 1], "s_rs", "r_dir", along(e))
            put(mine.at[ring(-e)], dirb.at[e + 2], "s_rs", "r_dir", along(-e))
        for k in FAR_RING:
            put(sca.at[z], sca.at[z], "s_sa", "r_sa", along(k))

        got(relp, "r_relp")
        part[c, ring(4)] = part[c, ring(4)] + jnp.sum(relp[...], axis=0)
        put(mine.at[ring(4)], fin.at[0], "s_rs", "r_fin", along(4))
        got(relm, "r_relm")
        part[c, ring(-4)] = part[c, ring(-4)] + jnp.sum(relm[...], axis=0)
        put(mine.at[ring(-4)], fin.at[1], "s_rs", "r_fin", along(-4))

        @pl.when(it == 0)
        def _():
            build_l()

        @pl.when(j < HALO)
        def _():
            got(gext.at[pl.ds(0, HALO)], "r_hl")
            sent(gext.at[pl.ds(0, HALO)], "s_hl")

        @pl.when(j >= XY - HALO)
        def _():
            got(gext.at[pl.ds(0, HALO)], "r_hr")
            sent(gext.at[pl.ds(0, HALO)], "s_hr")

        window = gext[pl.ds(j, XY)].reshape(JWIN, 128)
        lg = folded(dot(lx[...], halves(window)))
        rg = folded(dot(lxt[...], halves(lg)))[24 : 24 + R]

        got(sca.at[pl.ds(0, NZ - 1)], "r_sa")
        norm = jnp.sum(sca[...], axis=0)
        beta = norm / vals[1]
        vals[1] = norm
        got(dirb, "r_dir")
        got(fin, "r_fin")
        image = part[c, z] + jnp.sum(dirb[...], axis=0) + jnp.sum(fin[...], axis=0) + beta * imgown[...]
        imgown[...] = image

        @pl.when(it < ITERS - 1)
        def _():
            img[c, z] = image
            for e in (4, 3, 2, 1):
                for way in (e, -e):
                    r = {4: "r_aga", -4: "r_agb"}.get(way, "r_ag6")
                    put(img.at[c, z], img.at[c, z], "s_ag", r, along(way))

        ld = lg[160 : 160 + R] + beta * ldown[...]
        ldown[...] = ld
        rown[...] = rg + beta * rown[...]
        share = jnp.sum(image * image, axis=0, keepdims=True)
        share = share + weight[...] * weight[...] * jnp.sum(ld * ld, axis=0, keepdims=True)
        place = 2 * z + c
        scb[place] = share
        @pl.when(it < ITERS - 1)
        def _():
            got(img.at[c, 0], "r_aga")
            for e in (4, 3, 2, 1):
                put(img.at[c, ring(-4)], img.at[c, ring(-4)], "s_ag", "r_ag7", along(e))
            got(img.at[c, 0], "r_agb")
            for e in (3, 2, 1):
                put(img.at[c, ring(4)], img.at[c, ring(4)], "s_ag", "r_ag7", along(-e))

        for to in [along(k) for k in FAR_RING] + [(x, y, ring(k), 1 - c) for k in FAR_RING] + [partner]:
            put(scb.at[place], scb.at[place], "s_sb", "r_sb", to)

        def turn(i, _):
            d[i] = gext[HALO + i] + beta * d[i]
            return 0

        lax.fori_loop(0, XY, turn, 0)

        @pl.when(it < ITERS - 1)
        def _():
            got(img.at[c, pl.ds(0, 6)], "r_ag6")
            got(img.at[c, pl.ds(0, 7)], "r_ag7")
            put(img.at[c], img.at[c], "s_pag", "r_pag", partner)
            sent(img.at[c, pl.ds(0, 15)], "s_ag")

        sent(xyr.at[pl.ds(0, XY - 1)], "s_xy")
        @pl.when(it > 0)
        def _():
            sent(xs.at[pl.ds(0, XY - 1)], "s_xs")

        sent(gext.at[pl.ds(0, XY - 1)], "s_xg")
        sent(snd.at[0], "s_pa")
        sent(pairb, "s_pair")
        sent(pairb.at[pl.ds(0, NZ - 1)], "s_rs")
        sent(sca.at[pl.ds(0, NZ - 1)], "s_sa")
        sent(scb.at[pl.ds(0, 2 * NZ - 1)], "s_sb")
        return 0

    lax.fori_loop(0, ITERS, body, 0)

    exchange_curvature()
    step_on(vals[1] / curvature())
    sent(xs.at[pl.ds(0, XY - 1)], "s_xs")
    sent(offl.at[:, pl.ds(0, 2 * OFFH)], "s_off")


def shards(green, data, neighbours, reg_weight):
    rows, cols = green.shape
    chunks = (XY, R, 128)
    vmem = pl.BlockSpec(memory_space=pltpu.VMEM)
    hbm = pl.BlockSpec(memory_space=pltpu.HBM)
    scratch = [
        ((rows, cols), F32),
        ((rows, cols), BF16), ((rows, cols), BF16), ((2, cols, cols), BF16), ((2, cols, cols), BF16),
        ((640, 256), BF16), ((640, 256), BF16),
        ((2, *chunks), F32), (chunks, F32),
        ((4, R, 128), F32), ((3, R, 128), F32), ((6, R, 128), F32), ((2, R, 128), F32),
        ((2, *chunks), F32), (chunks, F32), (chunks, F32),
        ((2 * HALO + XY + 1, R, 128), F32), (chunks, F32),
        ((R, 128), F32), ((R, 128), F32), ((R, 128), F32),
        ((8, 2 * OFFH + cols), F32), ((KWIN, JWIN), BF16), ((128, KWIN), BF16),
        ((NZ, 1, 128), F32), ((2 * NZ, 1, 128), F32), ((XY, 1, 128), F32),
        ((1, 1, 128), F32), ((1, 1, 128), F32), ((2, 1, 128), F32),
    ]
    result = pl.pallas_call(
        kernel,
        out_shape=jax.ShapeDtypeStruct(chunks, F32),
        in_specs=[hbm] * 4,
        out_specs=vmem,
        scratch_shapes=[pltpu.VMEM(shape, kind) for shape, kind in scratch]
        + [pltpu.VMEM(neighbours.shape, jnp.int32), pltpu.VMEM((1, 128), F32), pltpu.SemaphoreType.DMA((len(SEMS),))],
        compiler_params=pltpu.CompilerParams(
            collective_id=0, has_side_effects=True, vmem_limit_bytes=67_000_000
        ),
    )(green, data.reshape(2, *chunks), neighbours, reg_weight.reshape(1, 128))
    return result.reshape(cols, 128)


def solution(mesh):
    whole = Mesh(mesh.devices.reshape(NX, NY, NZ, 2), ("x", "y", "z", "c"))
    in_specs = (P(OBS, PATCH), P(OBS, None), P(None, PATCH), P())
    return jax.shard_map(
        shards, mesh=whole, in_specs=in_specs, out_specs=P(PATCH, None), check_vma=False
    )
```

```python
import jax
import jax.numpy as jnp
from jax import lax
from jax.experimental import pallas as pl
from jax.experimental.pallas import tpu as pltpu
from jax.sharding import Mesh
from jax.sharding import PartitionSpec as P

ITERS = 3
NX, NY, NZ = 4, 4, 16
XY = NX * NY
OBS = ("x", "y")
PATCH = ("z", "c")
F32, BF16 = jnp.float32, jnp.bfloat16
MESH = pl.DeviceIdType.MESH

R = 40
HALO = 7
KWIN = 384
JWIN = 640
OFFH = 256

SEMS = (
    ["g0", "g1", "g2", "g3", "g4", "data", "nb", "w", "s_off", "r_offl", "r_offr", "s_xy", "r_xy", "s_xs", "r_xs", "s_xg", "r_xg"]
    + ["s_pa", "r_pa", "s_pair", "r_pair", "s_rs", "r_6p", "r_6m", "r_3p", "r_3m", "r_dir", "r_fin", "s_sa", "r_sa"]
    + ["s_hl", "s_hr", "r_hl", "r_hr", "s_ag", "r_a3p", "r_a3m", "r_a6p", "r_a6m", "r_ad", "r_ax", "s_sb", "r_sb"]
    + ["s_pag", "r_pag"]
)
SEM = {name: place for place, name in enumerate(SEMS)}


def hops(offset):
    return sum(min(step, size - step) for step, size in zip(offset, (NX, NY)))


FAR_RING = sorted(range(1, NZ), key=lambda k: min(k, NZ - k), reverse=True)
FARTHEST_FIRST = sorted(
    ((dx, dy) for dx in range(NX) for dy in range(NY) if dx or dy), key=hops, reverse=True
)


def split(value):
    high = value.astype(BF16)
    low = (value - high.astype(F32)).astype(BF16)
    return high, low


def halves(value):
    return jnp.concatenate(split(value), axis=-1)


def folded(value):
    return value[:, :128] + value[:, 128:]


def dot(a, b):
    return jnp.dot(a, b, preferred_element_type=F32)


def kernel(
    green, data, neighbours, reg_weight, out,
    gf, ghi, glo, thi, tlo, g2, im2, part, pairb, at6p, at6m, at3p, at3m, dirb, fin, img, q, xyr, gext, d,
    imgown, ldown, rown, offl, lx, lxt, sca, scb, xs, pab, snd, vals, table, weight, sems, known,
):
    x, y, z, c = (lax.axis_index(a) for a in ("x", "y", "z", "c"))
    j = x * NY + y
    sign = 1 - 2 * c
    partner = (x, y, z, 1 - c)

    def ring(step):
        return lax.rem(z + sign * step + 2 * NZ, NZ)

    def along(step):
        return (x, y, ring(step), c)

    def wrapped(place):
        return lax.rem(place + NZ, NZ)

    before = (x, y, wrapped(z - 1 + c), 1 - c)
    after = (x, y, wrapped(z + c), 1 - c)

    def plane():
        for dx, dy in FARTHEST_FIRST:
            px, py = lax.rem(x + dx, NX), lax.rem(y + dy, NY)
            yield px * NY + py, (px, py, z, c)

    def copy(src, dst, s, r, to):
        return pltpu.make_async_remote_copy(
            src_ref=src, dst_ref=dst, send_sem=sems.at[SEM[s]], recv_sem=sems.at[SEM[r]],
            device_id=to, device_id_type=MESH,
        )

    def put(src, dst, s, r, to):
        copy(src, dst, s, r, to).start()

    def got(ref, r):
        copy(ref, ref, "s_xy", r, partner).wait_recv()

    def sent(ref, s):
        copy(ref, ref, s, "r_xy", partner).wait_send()

    loads = [
        pltpu.make_async_copy(green.at[pl.ds(256 * i, 256)], gf.at[pl.ds(256 * i, 256)], sems.at[SEM["g0"] + i])
        for i in range(5)
    ]
    load_data = pltpu.make_async_copy(data, img, sems.at[SEM["data"]])
    load_table = pltpu.make_async_copy(neighbours, table, sems.at[SEM["nb"]])
    load_weight = pltpu.make_async_copy(reg_weight, weight, sems.at[SEM["w"]])
    load_table.start()
    for load in loads:
        load.start()
    load_data.start()
    load_weight.start()

    cols = neighbours.shape[1]
    base = (2 * z + c) * cols
    for ref in (gext, d, imgown, ldown, rown, sca, scb, xs, offl):
        ref[...] = jnp.zeros_like(ref)
    vals[0:1] = jnp.full((1, 1, 128), -1.0, F32)
    vals[1:2] = jnp.ones((1, 1, 128), F32)
    load_table.wait()
    ids = base + lax.broadcasted_iota(jnp.int32, table.shape, 1)
    offl[0:3, OFFH : OFFH + cols] = (table[...] - ids).astype(F32)

    barrier = pltpu.get_barrier_semaphore()
    greeted = [to for _, to in plane()] + [partner, along(1), along(-1)]
    greeted += [(x, y, wrapped(z - 1 + 2 * c), 1 - c)]
    for to in greeted:
        pl.semaphore_signal(barrier, inc=1, device_id=to, device_id_type=MESH)

    out[...] = jnp.zeros_like(out)
    for i in range(5):
        loads[i].wait()
        for k in range(2):
            place = 2 * i + k
            high, low = split(gf[pl.ds(128 * place, 128), :].T)
            half, columns = place // 5, pl.ds(128 * (place % 5), 128)
            thi[half, :, columns], tlo[half, :, columns] = high, low
    load_weight.wait()
    load_data.wait()

    def tell(doubling):
        for way in (1, -1):
            pl.semaphore_signal(known.at[doubling], inc=1, device_id=along(way * 2**doubling), device_id_type=MESH)

    def hear(doubling):
        pl.semaphore_wait(known.at[doubling], 2)

    def forward(half):
        def tile(i, _):
            rows = pl.ds(pl.multiple_of(half * 640 + i * 160, 160), 160)
            both = dot(ghi[rows, :], g2[...]) + dot(glo[rows, :], g2[...])
            part[half, pl.ds(4 * i, 4)] = folded(both).reshape(4, R, 128)
            return 0

        lax.fori_loop(0, 4, tile, 0)

    def back(half, last):
        def convert(i, _):
            rows = pl.ds(pl.multiple_of(i * 160, 160), 160)
            im2[rows, :] = halves(img[half, pl.ds(4 * i, 4)].reshape(160, 128))
            return 0

        lax.fori_loop(0, 4, convert, 0)
        def tile(i, _):
            side = lax.rem(x + 2 + i, NX)
            rows = pl.ds(pl.multiple_of(side * 160, 160), 160)
            both = dot(thi[half, rows, :], im2[...]) + dot(tlo[half, rows, :], im2[...])
            value = folded(both).reshape(NY, R, 128)
            place = pl.ds(NY * side, NY)
            q[place] = q[place] + value if last else value
            if last:
                for step in (2, 1, 3, 0):
                    py = lax.rem(y + step, NY)
                    other = NY * side + py

                    @pl.when(other != j)
                    def _():
                        put(q.at[other], xyr.at[j], "s_xy", "r_xy", (side, py, z, c))

            return 0

        lax.fori_loop(0, NX, tile, 0)

    def split_rows():
        def tile(i, _):
            rows = pl.ds(pl.multiple_of(i * 128, 128), 128)
            ghi[rows, :], glo[rows, :] = split(gf[rows, :])
            return 0

        lax.fori_loop(0, 10, tile, 0)

    def exchange_curvature():
        got(scb.at[pl.ds(0, 2 * NZ - 1)], "r_sb")
        xs[pl.ds(j, 1)] = jnp.sum(scb[...], axis=0, keepdims=True)
        for _, to in plane():
            put(xs.at[j], xs.at[j], "s_xs", "r_xs", to)

    def curvature():
        got(xs.at[pl.ds(0, XY - 1)], "r_xs")
        return jnp.sum(xs[...], axis=0)

    def step_on(scale):
        def add(i, _):
            out[i] = out[i] + scale * d[i]
            return 0

        lax.fori_loop(0, XY, add, 0)

    def build_l():
        got(offl.at[:, pl.ds(0, OFFH)], "r_offl")
        got(offl.at[:, pl.ds(0, OFFH)], "r_offr")
        pick = (
            lax.broadcasted_iota(jnp.int32, (8, 128), 0) == lax.broadcasted_iota(jnp.int32, (8, 128), 1)
        ).astype(F32)
        turned = lax.dot_general(
            offl[...].astype(BF16), pick.astype(BF16), (((0,), (0,)), ((), ())), preferred_element_type=F32
        )
        gf[0:1152, 0:128] = turned
        first = base + R * j - 160
        column = lax.broadcasted_iota(jnp.int32, (16, JWIN), 1).astype(F32)

        def rows16(i, _):
            shift = gf[pl.ds(pl.multiple_of(96 + R * j + 16 * i, 8), 16), 0:128]
            row = 16 * i + lax.broadcasted_iota(jnp.int32, (16, 1), 0)
            place = (row + 120).astype(F32)
            value = jnp.where(column == place, 4.0, 0.0)
            for slot in range(3):
                value = value - jnp.where(column == place + shift[:, slot : slot + 1], 1.0, 0.0)
            known = jnp.logical_and(first + row >= 0, first + row < cols * 2 * NZ)
            value = value * known.astype(F32)
            lx[pl.ds(pl.multiple_of(16 * i, 16), 16), :] = value.astype(BF16)
            return 0

        lax.fori_loop(0, KWIN // 16, rows16, 0)
        lxt[...] = lx[:, 256:384].astype(F32).T.astype(BF16)

    def body(it, _):
        back(c, False)

        @pl.when(it > 0)
        def _():
            got(img.at[0], "r_pag")

        @pl.when(it == 0)
        def _():
            pl.semaphore_wait(barrier, len(greeted))
            tell(0)
            put(offl.at[:, pl.ds(cols, OFFH)], offl.at[:, pl.ds(0, OFFH)], "s_off", "r_offl", after)
            put(offl.at[:, pl.ds(OFFH, OFFH)], offl.at[:, pl.ds(OFFH + cols, OFFH)], "s_off", "r_offr", before)

        back(1 - c, True)

        @pl.when(it > 0)
        def _():
            sent(img.at[0], "s_pag")

        xyr[j] = q[j]

        @pl.when(it > 0)
        def _():
            exchange_curvature()
            vals[0] = vals[1] / curvature()

        @pl.when(it == 0)
        def _():
            hear(0)
            tell(1)
            split_rows()

        alpha = vals[0]
        got(xyr.at[pl.ds(0, XY - 1)], "r_xy")
        total = jnp.sum(xyr[...], axis=0) + weight[...] * weight[...] * rown[...]
        gext[HALO + j] = gext[HALO + j] - alpha * total
        for _, to in plane():
            put(gext.at[HALO + j], gext.at[HALO + j], "s_xg", "r_xg", to)
        @pl.when(it == 0)
        def _():
            hear(1)
            tell(2)

        step_on(alpha)
        got(gext.at[pl.ds(0, XY - 1)], "r_xg")

        @pl.when(it == 0)
        def _():
            hear(2)

        @pl.when(j < HALO)
        def _():
            put(gext.at[pl.ds(XY, HALO)], gext.at[pl.ds(0, HALO)], "s_hl", "r_hl", after)

        @pl.when(j >= XY - HALO)
        def _():
            put(gext.at[pl.ds(HALO, HALO)], gext.at[pl.ds(HALO + XY, HALO)], "s_hr", "r_hr", before)

        def convert(i, square):
            value = gext[pl.ds(HALO + 4 * i, 4)].reshape(160, 128)
            g2[pl.ds(pl.multiple_of(160 * i, 160), 160), :] = halves(value)
            return square + jnp.sum(value * value, axis=0, keepdims=True)

        square = lax.fori_loop(0, 4, convert, jnp.zeros((1, 128), F32))
        snd[0] = square
        put(snd.at[0], pab.at[0], "s_pa", "r_pa", partner)
        forward(1 - c)
        put(part.at[1 - c], pairb, "s_pair", "r_pair", partner)
        got(pab.at[0], "r_pa")
        sca[z] = square + pab[0]
        for k in FAR_RING:
            put(sca.at[z], sca.at[z], "s_sa", "r_sa", along(k))
        forward(c)
        got(pairb, "r_pair")

        def add_pair(i, _):
            part[c, i] = part[c, i] + pairb[i]
            return 0

        lax.fori_loop(0, NZ, add_pair, 0)

        mine = part.at[c]
        relays = ((1, 6, at6p, "r_6p"), (-1, 6, at6m, "r_6m"), (1, 3, at3p, "r_3p"), (-1, 3, at3m, "r_3m"))
        for way, near, held, name in relays:
            for e in range(near + held.shape[0], near, -1):
                put(mine.at[ring(way * e)], held.at[e - near - 1], "s_rs", name, along(way * (e - near)))
        for e in (2, 1):
            for way in (1, -1):
                put(mine.at[ring(way * e)], dirb.at[e - way], "s_rs", "r_dir", along(way * e))
        for place, (way, near, held, name) in enumerate(relays):
            got(held, name)
            target = ring(way * near)
            part[c, target] = part[c, target] + jnp.sum(held[...], axis=0)
            put(mine.at[target], fin.at[place], "s_rs", "r_fin", along(way * near))

        @pl.when(it == 0)
        def _():
            build_l()

        @pl.when(j < HALO)
        def _():
            got(gext.at[pl.ds(0, HALO)], "r_hl")
            sent(gext.at[pl.ds(0, HALO)], "s_hl")

        @pl.when(j >= XY - HALO)
        def _():
            got(gext.at[pl.ds(0, HALO)], "r_hr")
            sent(gext.at[pl.ds(0, HALO)], "s_hr")

        window = gext[pl.ds(j, XY)].reshape(JWIN, 128)
        lg = folded(dot(lx[...], halves(window)))
        rg = folded(dot(lxt[...], halves(lg)))[24 : 24 + R]

        got(sca.at[pl.ds(0, NZ - 1)], "r_sa")
        norm = jnp.sum(sca[...], axis=0)
        beta = norm / vals[1]
        vals[1] = norm
        got(dirb, "r_dir")
        got(fin, "r_fin")
        image = part[c, z] + jnp.sum(dirb[...], axis=0) + jnp.sum(fin[...], axis=0) + beta * imgown[...]
        imgown[...] = image

        @pl.when(it < ITERS - 1)
        def _():
            img[c, z] = image
            for e, name in ((6, "r_a6"), (3, "r_a3"), (2, "r_ad"), (1, "r_ad")):
                for way, side in ((1, "p"), (-1, "m")):
                    put(img.at[c, z], img.at[c, z], "s_ag", name + side if e > 2 else name, along(way * e))

        ld = lg[160 : 160 + R] + beta * ldown[...]
        ldown[...] = ld
        rown[...] = rg + beta * rown[...]
        share = jnp.sum(image * image, axis=0, keepdims=True)
        share = share + weight[...] * weight[...] * jnp.sum(ld * ld, axis=0, keepdims=True)
        place = 2 * z + c
        scb[place] = share
        @pl.when(it < ITERS - 1)
        def _():
            for way, far, last, name in ((1, 3, 2, "r_a3p"), (-1, 3, 2, "r_a3m"), (1, 6, 2, "r_a6p"), (-1, 6, 1, "r_a6m")):
                got(img.at[c, 0], name)
                held = img.at[c, ring(-far * way)]
                for e in range(last, 0, -1):
                    put(held, held, "s_ag", "r_ax", along(way * e))

        for to in [along(k) for k in FAR_RING] + [(x, y, ring(k), 1 - c) for k in FAR_RING] + [partner]:
            put(scb.at[place], scb.at[place], "s_sb", "r_sb", to)

        def turn(i, _):
            d[i] = gext[HALO + i] + beta * d[i]
            return 0

        lax.fori_loop(0, XY, turn, 0)

        @pl.when(it < ITERS - 1)
        def _():
            got(img.at[c, pl.ds(0, 4)], "r_ad")
            got(img.at[c, pl.ds(0, 7)], "r_ax")
            put(img.at[c], img.at[c], "s_pag", "r_pag", partner)
            sent(img.at[c, pl.ds(0, 15)], "s_ag")

        sent(xyr.at[pl.ds(0, XY - 1)], "s_xy")
        @pl.when(it > 0)
        def _():
            sent(xs.at[pl.ds(0, XY - 1)], "s_xs")

        sent(gext.at[pl.ds(0, XY - 1)], "s_xg")
        sent(snd.at[0], "s_pa")
        sent(pairb, "s_pair")
        sent(pairb.at[pl.ds(0, NZ - 1)], "s_rs")
        sent(sca.at[pl.ds(0, NZ - 1)], "s_sa")
        sent(scb.at[pl.ds(0, 2 * NZ - 1)], "s_sb")
        return 0

    lax.fori_loop(0, ITERS, body, 0)

    exchange_curvature()
    step_on(vals[1] / curvature())
    sent(xs.at[pl.ds(0, XY - 1)], "s_xs")
    sent(offl.at[:, pl.ds(0, 2 * OFFH)], "s_off")


def shards(green, data, neighbours, reg_weight):
    rows, cols = green.shape
    chunks = (XY, R, 128)
    vmem = pl.BlockSpec(memory_space=pltpu.VMEM)
    hbm = pl.BlockSpec(memory_space=pltpu.HBM)
    scratch = [
        ((rows, cols), F32),
        ((rows, cols), BF16), ((rows, cols), BF16), ((2, cols, cols), BF16), ((2, cols, cols), BF16),
        ((640, 256), BF16), ((640, 256), BF16),
        ((2, *chunks), F32), (chunks, F32),
        ((2, R, 128), F32), ((1, R, 128), F32), ((2, R, 128), F32), ((2, R, 128), F32),
        ((4, R, 128), F32), ((4, R, 128), F32),
        ((2, *chunks), F32), (chunks, F32), (chunks, F32),
        ((2 * HALO + XY + 1, R, 128), F32), (chunks, F32),
        ((R, 128), F32), ((R, 128), F32), ((R, 128), F32),
        ((8, 2 * OFFH + cols), F32), ((KWIN, JWIN), BF16), ((128, KWIN), BF16),
        ((NZ, 1, 128), F32), ((2 * NZ, 1, 128), F32), ((XY, 1, 128), F32),
        ((1, 1, 128), F32), ((1, 1, 128), F32), ((2, 1, 128), F32),
    ]
    result = pl.pallas_call(
        kernel,
        out_shape=jax.ShapeDtypeStruct(chunks, F32),
        in_specs=[hbm] * 4,
        out_specs=vmem,
        scratch_shapes=[pltpu.VMEM(shape, kind) for shape, kind in scratch]
        + [pltpu.VMEM(neighbours.shape, jnp.int32), pltpu.VMEM((1, 128), F32), pltpu.SemaphoreType.DMA((len(SEMS),)), pltpu.SemaphoreType.REGULAR((3,))],
        compiler_params=pltpu.CompilerParams(
            collective_id=0, has_side_effects=True, vmem_limit_bytes=67_000_000
        ),
    )(green, data.reshape(2, *chunks), neighbours, reg_weight.reshape(1, 128))
    return result.reshape(cols, 128)


def solution(mesh):
    whole = Mesh(mesh.devices.reshape(NX, NY, NZ, 2), ("x", "y", "z", "c"))
    in_specs = (P(OBS, PATCH), P(OBS, None), P(None, PATCH), P())
    return jax.shard_map(
        shards, mesh=whole, in_specs=in_specs, out_specs=P(PATCH, None), check_vma=False
    )
```

```python
import jax
import jax.numpy as jnp
from jax import lax
from jax.experimental import pallas as pl
from jax.experimental.pallas import tpu as pltpu
from jax.sharding import Mesh
from jax.sharding import PartitionSpec as P

ITERS = 3
NX, NY, NZ = 4, 4, 16
XY = NX * NY
OBS = ("x", "y")
PATCH = ("z", "c")
F32, BF16 = jnp.float32, jnp.bfloat16
MESH = pl.DeviceIdType.MESH

R = 40
HALO = 7
KWIN = 384
JWIN = 640
OFFH = 256

SEMS = (
    ["g0", "g1", "g2", "g3", "g4", "data", "nb", "w", "s_off", "r_offl", "r_offr", "s_xy", "r_xy", "s_xs", "r_xs", "s_xg", "r_xg"]
    + ["s_pa", "r_pa", "s_pair", "r_pair", "s_rs", "r_5p", "r_5m", "r_2p", "r_2m", "r_dir", "r_fin", "s_sa", "r_sa"]
    + ["s_hl", "s_hr", "r_hl", "r_hr", "s_ag", "r_a2p", "r_a2m", "r_a5p", "r_a5m", "r_ad", "r_ax", "s_sb", "r_sb"]
    + ["s_pag", "r_pag"]
)
SEM = {name: place for place, name in enumerate(SEMS)}


def hops(offset):
    return sum(min(step, size - step) for step, size in zip(offset, (NX, NY)))


FAR_RING = sorted(range(1, NZ), key=lambda k: min(k, NZ - k), reverse=True)
FARTHEST_FIRST = sorted(
    ((dx, dy) for dx in range(NX) for dy in range(NY) if dx or dy), key=hops, reverse=True
)


def split(value):
    high = value.astype(BF16)
    low = (value - high.astype(F32)).astype(BF16)
    return high, low


def halves(value):
    return jnp.concatenate(split(value), axis=-1)


def folded(value):
    return value[:, :128] + value[:, 128:]


def dot(a, b):
    return jnp.dot(a, b, preferred_element_type=F32)


def kernel(
    green, data, neighbours, reg_weight, out,
    gf, ghl, thl, g2, im2, part, pairb, at5p, at5m, at2p, at2m, dirb, fin, img, q, xyr, gext, d,
    imgown, ldown, rown, offl, lx, lxt, sca, scb, xs, pab, snd, vals, table, weight, sems, known,
):
    x, y, z, c = (lax.axis_index(a) for a in ("x", "y", "z", "c"))
    j = x * NY + y
    sign = 1 - 2 * c
    partner = (x, y, z, 1 - c)

    places = [lax.rem(z + sign * step + NZ, NZ) for step in range(NZ)]

    def ring(step):
        return places[step % NZ]

    def along(step):
        return (x, y, ring(step), c)

    def wrapped(place):
        return lax.rem(place + NZ, NZ)

    before = (x, y, wrapped(z - 1 + c), 1 - c)
    after = (x, y, wrapped(z + c), 1 - c)

    xs_of = [lax.rem(x + step, NX) for step in range(NX)]
    ys_of = [lax.rem(y + step, NY) for step in range(NY)]

    def plane():
        for dx, dy in FARTHEST_FIRST:
            px, py = xs_of[dx], ys_of[dy]
            yield px * NY + py, (px, py, z, c)

    def copy(src, dst, s, r, to):
        return pltpu.make_async_remote_copy(
            src_ref=src, dst_ref=dst, send_sem=sems.at[SEM[s]], recv_sem=sems.at[SEM[r]],
            device_id=to, device_id_type=MESH,
        )

    def put(src, dst, s, r, to):
        copy(src, dst, s, r, to).start()

    def got(ref, r):
        copy(ref, ref, "s_xy", r, partner).wait_recv()

    def sent(ref, s):
        copy(ref, ref, s, "r_xy", partner).wait_send()

    loads = [
        pltpu.make_async_copy(green.at[pl.ds(256 * i, 256)], gf.at[pl.ds(256 * i, 256)], sems.at[SEM["g0"] + i])
        for i in range(5)
    ]
    load_data = pltpu.make_async_copy(data, img, sems.at[SEM["data"]])
    load_table = pltpu.make_async_copy(neighbours, table, sems.at[SEM["nb"]])
    load_weight = pltpu.make_async_copy(reg_weight, weight, sems.at[SEM["w"]])
    load_table.start()
    for load in loads:
        load.start()
    load_data.start()
    load_weight.start()

    cols = neighbours.shape[1]
    base = (2 * z + c) * cols
    for ref in (gext, d, imgown, ldown, rown, sca, scb, xs, offl):
        ref[...] = jnp.zeros_like(ref)
    vals[0:1] = jnp.full((1, 1, 128), -1.0, F32)
    vals[1:2] = jnp.ones((1, 1, 128), F32)
    load_table.wait()
    ids = base + lax.broadcasted_iota(jnp.int32, table.shape, 1)
    offl[0:3, OFFH : OFFH + cols] = (table[...] - ids).astype(F32)

    barrier = pltpu.get_barrier_semaphore()
    greeted = [to for _, to in plane()] + [partner, along(1), along(-1)]
    greeted += [(x, y, wrapped(z - 1 + 2 * c), 1 - c)]
    for to in greeted:
        pl.semaphore_signal(barrier, inc=1, device_id=to, device_id_type=MESH)

    out[...] = jnp.zeros_like(out)
    for i in range(5):
        loads[i].wait()
        for k in range(2):
            place = 2 * i + k
            high, low = split(gf[pl.ds(128 * place, 128), :].T)
            half, first = place // 5, 128 * (place % 5)
            thl[half, :, pl.ds(first, 128)], thl[half, :, pl.ds(cols + first, 128)] = high, low
    load_weight.wait()
    load_data.wait()

    def tell(doubling):
        for way in (1, -1):
            pl.semaphore_signal(known.at[doubling], inc=1, device_id=along(way * 2**doubling), device_id_type=MESH)

    def hear(doubling):
        pl.semaphore_wait(known.at[doubling], 2)

    def forward(half):
        def tile(i, _):
            rows = pl.ds(pl.multiple_of(half * 640 + i * 320, 320), 320)
            both = dot(ghl[rows, :], g2[...])
            part[half, pl.ds(8 * i, 8)] = folded(both).reshape(8, R, 128)
            return 0

        lax.fori_loop(0, 2, tile, 0)

    def back(half, last):
        def convert(i, _):
            rows = pl.ds(pl.multiple_of(i * 160, 160), 160)
            pieces = halves(img[half, pl.ds(4 * i, 4)].reshape(160, 128))
            im2[rows, :] = pieces
            im2[pl.ds(pl.multiple_of(cols + i * 160, 160), 160), :] = pieces
            return 0

        lax.fori_loop(0, 4, convert, 0)
        def tile(i, _):
            side = lax.rem(x + 2 + i, NX)
            rows = pl.ds(pl.multiple_of(side * 160, 160), 160)
            both = dot(thl[half, rows, :], im2[...])
            value = folded(both).reshape(NY, R, 128)
            place = pl.ds(NY * side, NY)
            q[place] = q[place] + value if last else value
            if last:
                for step in (2, 1, 3, 0):
                    py = ys_of[step]
                    other = NY * side + py

                    @pl.when(other != j)
                    def _():
                        put(q.at[other], xyr.at[j], "s_xy", "r_xy", (side, py, z, c))

            return 0

        lax.fori_loop(0, NX, tile, 0)

    def split_rows():
        def tile(i, _):
            rows = pl.ds(pl.multiple_of(i * 128, 128), 128)
            ghl[rows, :] = halves(gf[rows, :])
            return 0

        lax.fori_loop(0, 10, tile, 0)

    def exchange_curvature():
        got(scb.at[pl.ds(0, 2 * NZ - 1)], "r_sb")
        xs[pl.ds(j, 1)] = jnp.sum(scb[...], axis=0, keepdims=True)
        for _, to in plane():
            put(xs.at[j], xs.at[j], "s_xs", "r_xs", to)

    def curvature():
        got(xs.at[pl.ds(0, XY - 1)], "r_xs")
        return jnp.sum(xs[...], axis=0)

    def step_on(scale):
        def add(i, _):
            out[i] = out[i] + scale * d[i]
            return 0

        lax.fori_loop(0, XY, add, 0)

    def build_l():
        got(offl.at[:, pl.ds(0, OFFH)], "r_offl")
        got(offl.at[:, pl.ds(0, OFFH)], "r_offr")
        pick = (
            lax.broadcasted_iota(jnp.int32, (8, 128), 0) == lax.broadcasted_iota(jnp.int32, (8, 128), 1)
        ).astype(F32)
        turned = lax.dot_general(
            offl[...].astype(BF16), pick.astype(BF16), (((0,), (0,)), ((), ())), preferred_element_type=F32
        )
        gf[0:1152, 0:128] = turned
        first = base + R * j - 160
        column = lax.broadcasted_iota(jnp.int32, (16, JWIN), 1).astype(F32)

        def rows16(i, _):
            shift = gf[pl.ds(pl.multiple_of(96 + R * j + 16 * i, 8), 16), 0:128]
            row = 16 * i + lax.broadcasted_iota(jnp.int32, (16, 1), 0)
            place = (row + 120).astype(F32)
            value = jnp.where(column == place, 4.0, 0.0)
            for slot in range(3):
                value = value - jnp.where(column == place + shift[:, slot : slot + 1], 1.0, 0.0)
            known = jnp.logical_and(first + row >= 0, first + row < cols * 2 * NZ)
            value = value * known.astype(F32)
            lx[pl.ds(pl.multiple_of(16 * i, 16), 16), :] = value.astype(BF16)
            return 0

        lax.fori_loop(0, KWIN // 16, rows16, 0)
        lxt[...] = lx[:, 256:384].astype(F32).T.astype(BF16)

    def body(it, _):
        back(c, False)

        @pl.when(it > 0)
        def _():
            got(img.at[0], "r_pag")

        @pl.when(it == 0)
        def _():
            pl.semaphore_wait(barrier, len(greeted))
            tell(0)
            put(offl.at[:, pl.ds(cols, OFFH)], offl.at[:, pl.ds(0, OFFH)], "s_off", "r_offl", after)
            put(offl.at[:, pl.ds(OFFH, OFFH)], offl.at[:, pl.ds(OFFH + cols, OFFH)], "s_off", "r_offr", before)

        back(1 - c, True)

        @pl.when(it > 0)
        def _():
            sent(img.at[0], "s_pag")

        xyr[j] = q[j]

        @pl.when(it > 0)
        def _():
            exchange_curvature()
            vals[0] = vals[1] / curvature()

        @pl.when(it == 0)
        def _():
            hear(0)
            tell(1)
            split_rows()

        alpha = vals[0]
        got(xyr.at[pl.ds(0, XY - 1)], "r_xy")
        total = jnp.sum(xyr[...], axis=0) + weight[...] * weight[...] * rown[...]
        gext[HALO + j] = gext[HALO + j] - alpha * total
        for _, to in plane():
            put(gext.at[HALO + j], gext.at[HALO + j], "s_xg", "r_xg", to)
        @pl.when(it == 0)
        def _():
            hear(1)
            tell(2)

        step_on(alpha)
        got(gext.at[pl.ds(0, XY - 1)], "r_xg")

        @pl.when(it == 0)
        def _():
            hear(2)

        @pl.when(j < HALO)
        def _():
            put(gext.at[pl.ds(XY, HALO)], gext.at[pl.ds(0, HALO)], "s_hl", "r_hl", after)

        @pl.when(j >= XY - HALO)
        def _():
            put(gext.at[pl.ds(HALO, HALO)], gext.at[pl.ds(HALO + XY, HALO)], "s_hr", "r_hr", before)

        def convert(i, square):
            value = gext[pl.ds(HALO + 4 * i, 4)].reshape(160, 128)
            pieces = halves(value)
            g2[pl.ds(pl.multiple_of(160 * i, 160), 160), :] = pieces
            g2[pl.ds(pl.multiple_of(cols + 160 * i, 160), 160), :] = pieces
            return square + jnp.sum(value * value, axis=0, keepdims=True)

        square = lax.fori_loop(0, 4, convert, jnp.zeros((1, 128), F32))
        snd[0] = square
        put(snd.at[0], pab.at[0], "s_pa", "r_pa", partner)
        forward(1 - c)
        put(part.at[1 - c], pairb, "s_pair", "r_pair", partner)
        got(pab.at[0], "r_pa")
        sca[z] = square + pab[0]
        for k in FAR_RING:
            put(sca.at[z], sca.at[z], "s_sa", "r_sa", along(k))
        forward(c)
        got(pairb, "r_pair")

        mine = part.at[c]
        relays = ((1, 5, at5p, "r_5p"), (-1, 5, at5m, "r_5m"), (1, 2, at2p, "r_2p"), (-1, 2, at2m, "r_2m"))
        for way, near, held, name in relays:
            for e in range(near + held.shape[0], near, -1):
                part[c, ring(way * e)] = part[c, ring(way * e)] + pairb[ring(way * e)]
                put(mine.at[ring(way * e)], held.at[e - near - 1], "s_rs", name, along(way * (e - near)))
        for place, way in enumerate((1, -1)):
            part[c, ring(way)] = part[c, ring(way)] + pairb[ring(way)]
            put(mine.at[ring(way)], dirb.at[place], "s_rs", "r_dir", along(way))
        for place, (way, near, held, name) in enumerate(relays):
            got(held, name)
            target = ring(way * near)
            part[c, target] = part[c, target] + (pairb[target] + jnp.sum(held[...], axis=0))
            put(mine.at[target], fin.at[place], "s_rs", "r_fin", along(way * near))

        @pl.when(it == 0)
        def _():
            build_l()

        @pl.when(j < HALO)
        def _():
            got(gext.at[pl.ds(0, HALO)], "r_hl")
            sent(gext.at[pl.ds(0, HALO)], "s_hl")

        @pl.when(j >= XY - HALO)
        def _():
            got(gext.at[pl.ds(0, HALO)], "r_hr")
            sent(gext.at[pl.ds(0, HALO)], "s_hr")

        window = gext[pl.ds(j, XY)].reshape(JWIN, 128)
        lg = folded(dot(lx[...], halves(window)))
        rg = folded(dot(lxt[...], halves(lg)))[24 : 24 + R]

        got(sca.at[pl.ds(0, NZ - 1)], "r_sa")
        norm = jnp.sum(sca[...], axis=0)
        beta = norm / vals[1]
        vals[1] = norm
        got(dirb, "r_dir")
        got(fin, "r_fin")
        image = part[c, z] + pairb[z] + jnp.sum(dirb[...], axis=0) + jnp.sum(fin[...], axis=0) + beta * imgown[...]
        imgown[...] = image

        @pl.when(it < ITERS - 1)
        def _():
            img[c, z] = image
            for e, name in ((5, "r_a5"), (2, "r_a2"), (1, "r_ad")):
                for way, side in ((1, "p"), (-1, "m")):
                    put(img.at[c, z], img.at[c, z], "s_ag", name + side if e > 1 else name, along(way * e))

        ld = lg[160 : 160 + R] + beta * ldown[...]
        ldown[...] = ld
        rown[...] = rg + beta * rown[...]
        share = jnp.sum(image * image, axis=0, keepdims=True)
        share = share + weight[...] * weight[...] * jnp.sum(ld * ld, axis=0, keepdims=True)
        place = 2 * z + c
        scb[place] = share
        @pl.when(it < ITERS - 1)
        def _():
            for way, far, last, name in ((1, 2, 2, "r_a2p"), (-1, 2, 2, "r_a2m"), (1, 5, 3, "r_a5p"), (-1, 5, 2, "r_a5m")):
                got(img.at[c, 0], name)
                held = img.at[c, ring(-far * way)]
                for e in range(last, 0, -1):
                    put(held, held, "s_ag", "r_ax", along(way * e))

        for to in [along(k) for k in FAR_RING] + [(x, y, ring(k), 1 - c) for k in FAR_RING] + [partner]:
            put(scb.at[place], scb.at[place], "s_sb", "r_sb", to)

        def turn(i, _):
            d[i] = gext[HALO + i] + beta * d[i]
            return 0

        lax.fori_loop(0, XY, turn, 0)

        @pl.when(it < ITERS - 1)
        def _():
            got(img.at[c, pl.ds(0, 2)], "r_ad")
            for e in (0, 1, -1, 2, -2, 5, -5):
                put(img.at[c, ring(e)], img.at[c, ring(e)], "s_pag", "r_pag", partner)
            got(img.at[c, pl.ds(0, 9)], "r_ax")
            for e in (3, -3, 4, -4, 6, -6, 7, -7, 8):
                put(img.at[c, ring(e)], img.at[c, ring(e)], "s_pag", "r_pag", partner)
            sent(img.at[c, pl.ds(0, 15)], "s_ag")

        sent(xyr.at[pl.ds(0, XY - 1)], "s_xy")
        @pl.when(it > 0)
        def _():
            sent(xs.at[pl.ds(0, XY - 1)], "s_xs")

        sent(gext.at[pl.ds(0, XY - 1)], "s_xg")
        sent(snd.at[0], "s_pa")
        sent(pairb, "s_pair")
        sent(pairb.at[pl.ds(0, NZ - 1)], "s_rs")
        sent(sca.at[pl.ds(0, NZ - 1)], "s_sa")
        sent(scb.at[pl.ds(0, 2 * NZ - 1)], "s_sb")
        return 0

    lax.fori_loop(0, ITERS, body, 0)

    exchange_curvature()
    step_on(vals[1] / curvature())
    sent(xs.at[pl.ds(0, XY - 1)], "s_xs")
    sent(offl.at[:, pl.ds(0, 2 * OFFH)], "s_off")


def shards(green, data, neighbours, reg_weight):
    rows, cols = green.shape
    chunks = (XY, R, 128)
    vmem = pl.BlockSpec(memory_space=pltpu.VMEM)
    hbm = pl.BlockSpec(memory_space=pltpu.HBM)
    scratch = [
        ((rows, cols), F32),
        ((rows, 2 * cols), BF16), ((2, cols, 2 * cols), BF16),
        ((2 * cols, 256), BF16), ((2 * cols, 256), BF16),
        ((2, *chunks), F32), (chunks, F32),
        ((3, R, 128), F32), ((2, R, 128), F32), ((2, R, 128), F32), ((2, R, 128), F32),
        ((2, R, 128), F32), ((4, R, 128), F32),
        ((2, *chunks), F32), (chunks, F32), (chunks, F32),
        ((2 * HALO + XY + 1, R, 128), F32), (chunks, F32),
        ((R, 128), F32), ((R, 128), F32), ((R, 128), F32),
        ((8, 2 * OFFH + cols), F32), ((KWIN, JWIN), BF16), ((128, KWIN), BF16),
        ((NZ, 1, 128), F32), ((2 * NZ, 1, 128), F32), ((XY, 1, 128), F32),
        ((1, 1, 128), F32), ((1, 1, 128), F32), ((2, 1, 128), F32),
    ]
    result = pl.pallas_call(
        kernel,
        out_shape=jax.ShapeDtypeStruct(chunks, F32),
        in_specs=[hbm] * 4,
        out_specs=vmem,
        scratch_shapes=[pltpu.VMEM(shape, kind) for shape, kind in scratch]
        + [pltpu.VMEM(neighbours.shape, jnp.int32), pltpu.VMEM((1, 128), F32), pltpu.SemaphoreType.DMA((len(SEMS),)), pltpu.SemaphoreType.REGULAR((3,))],
        compiler_params=pltpu.CompilerParams(
            collective_id=0, has_side_effects=True, vmem_limit_bytes=67_000_000
        ),
    )(green, data.reshape(2, *chunks), neighbours, reg_weight.reshape(1, 128))
    return result.reshape(cols, 128)


def solution(mesh):
    whole = Mesh(mesh.devices.reshape(NX, NY, NZ, 2), ("x", "y", "z", "c"))
    in_specs = (P(OBS, PATCH), P(OBS, None), P(None, PATCH), P())
    return jax.shard_map(
        shards, mesh=whole, in_specs=in_specs, out_specs=P(PATCH, None), check_vma=False
    )
```
